32 devices in a mesh: lat: 4 (over x, core), lon: 8 (over z, y).
Axes of the slice: x: 2, y: 2, z: 4, core: 2. Of those that a mesh axis runs over, the one named last changes fastest.
Arguments:
- prediction_fields: float32 [4, 69, 360, 512], P(None, None, 'lon', 'lat'), may hold values from -16 to 16
- verifying_state: float32 [69, 360, 512], P(None, 'lon', 'lat'), may hold values from -16 to 16
- normal_state: float32 [69, 360, 512], P(None, 'lon', 'lat'), may hold values from -16 to 16
- evaluated_point_flag: int32 [360, 512], P('lon', 'lat'), may hold values 0 or 1
- parallels_each_strip: int32 [4], replicated, may hold values from 1 to 128, 361 in all
Outputs:
- parallel_quadratic_error: float32 [4, 69, 512], P(None, None, 'lat')
- parallel_systematic_error: float32 [4, 69, 512], P(None, None, 'lat')
- parallel_pattern_skill: float32 [4, 69, 512], P(None, None, 'lat')
- rmse: float32 [4, 69], replicated
- systematic_error: float32 [4, 69], replicated
- pattern_skill: float32 [4, 69], replicated
The draws below stay inside these ranges and needn't reach their ends.
Inputs may be any that keep to these rules, and one draw needn't show every extreme that they name: `parallels_each_strip`: they sum to 361, and some band holds exactly 128 rows.
All inputs are finite; a program needn't handle non-finite values.
Results may differ from the reference program's by a relative error of at most 0.00002.
Values sent between devices are 32-bit elements.
No kernel may reach another device: no remote copies, remote signals or barrier semaphores. Data moves between devices by JAX's collectives and lax.ppermute only.
A program may use at most 64 MiB of HBM per device.

```python
import math
import jax
import jax.numpy as jnp
import numpy as np
from jax import lax

VARS = 69
LEADS = 4
LAT_CAP = 128
LAT_BANDS = 4
NLAT = 361
EAST_WEST_SIZE = 360
LAT_BUF = 512


def common_fields(key):
    subkeys = jax.random.split(jax.random.fold_in(key, 4242), 8)
    climate = jax.random.normal(subkeys[0], (VARS, EAST_WEST_SIZE, LAT_BUF), jnp.float32)
    amplitude = jnp.exp(jax.random.uniform(subkeys[1], (VARS, 1, LAT_BUF), jnp.float32, jnp.log(0.5), jnp.log(2.0)))
    anomaly = jax.random.normal(subkeys[2], (VARS, EAST_WEST_SIZE, LAT_BUF), jnp.float32) * amplitude
    observed = climate + anomaly
    skill = jax.random.uniform(subkeys[4], (LEADS, VARS, 1, 1), jnp.float32, 0.3, 0.95)
    noise_scale = jax.random.uniform(subkeys[5], (LEADS, VARS, 1, 1), jnp.float32, 0.6, 1.2)
    drift = jax.random.uniform(subkeys[6], (LEADS, VARS, 1, LAT_BUF), jnp.float32, -0.6, 0.6)
    noise = jax.random.normal(subkeys[7], (LEADS, VARS, EAST_WEST_SIZE, LAT_BUF), jnp.float32)
    predicted = climate[None] + skill * anomaly[None] + noise_scale * amplitude[None] * noise + drift
    return (jnp.clip(predicted, -16.0, 16.0), jnp.clip(observed, -16.0, 16.0), jnp.clip(climate, -16.0, 16.0))


def draw_prediction_fields(key, part):
    return common_fields(key)[0]


def draw_verifying_state(key, part):
    return common_fields(key)[1]


def draw_normal_state(key, part):
    return common_fields(key)[2]


def place_ends(values, own_key, least, top_value):
    extent = values.shape
    index_at = [jax.random.randint(jax.random.fold_in(own_key, axis), (), 0, extent[axis]) for axis in range(len(extent))]
    values = values.at[tuple(index_at)].set(least)
    longest = extent.index(max(extent))
    index_at[longest] = (index_at[longest] + 1) % extent[longest]
    return values.at[tuple(index_at)].set(top_value)


def length_profile(count, total, limit, skew):
    portions = [(1 << 20) // math.isqrt(grade ** skew) + 1 for grade in range(2, count + 1)]
    spare, given = total - limit - (count - 1), [1] * (count - 1)
    while spare > 0:
        free = [i for i in range(count - 1) if given[i] < limit]
        mass, remaining = sum([portions[i] for i in free]), spare
        for i in free:
            extra = min(limit - given[i], max(1, remaining * portions[i] // mass), spare)
            given[i] = given[i] + extra
            spare = spare - extra
    return np.array([limit] + given)


def ragged(own_key, number_of, total, most, slope):
    if number_of == 2:
        one = jax.random.randint(own_key, (), max(1, total - most), min(most, total - 1) + 1)
        return jnp.stack([one, total - one])
    sizes = jnp.asarray(length_profile(number_of, total, most, slope), jnp.int32)
    twos = (number_of - 1) // 2
    donor, taker = sizes[1:1 + 2 * twos:2], sizes[2:2 + 2 * twos:2]
    margin = jnp.minimum(donor - 1, most - taker)
    passed = jax.random.randint(jax.random.fold_in(own_key, 1), (twos,), 0, 1 << 20) % (margin + 1)
    sizes = sizes.at[1:1 + 2 * twos:2].set(donor - passed).at[2:2 + 2 * twos:2].set(taker + passed)
    return sizes[jax.random.permutation(jax.random.fold_in(own_key, 2), number_of)]


def setup_inputs(seed: int = 0) -> dict:
    arg_keys = jax.random.split(jax.random.key(seed), 6)
    return {
        "prediction_fields": draw_prediction_fields(jax.random.fold_in(arg_keys[5], 71), 0),
        "verifying_state": draw_verifying_state(jax.random.fold_in(arg_keys[5], 71), 0),
        "normal_state": draw_normal_state(jax.random.fold_in(arg_keys[5], 71), 0),
        "evaluated_point_flag": place_ends((jax.random.randint(arg_keys[3], (EAST_WEST_SIZE, LAT_BUF), 0, 4) < 3).astype(jnp.int32), jax.random.fold_in(arg_keys[3], 1), 0, 1),
        "parallels_each_strip": ragged(arg_keys[4], LAT_BANDS, NLAT, LAT_CAP, 2).astype(jnp.int32),
    }


minimum_divisor = 0.1

def final_result(error_power_two, prediction_error, paired_anomaly_term, predicted_spread_sum, observed_dispersion, grid_point_tally):
    mean_square = error_power_two / grid_point_tally
    average_error = prediction_error / grid_point_tally
    covariance_sum = paired_anomaly_term / grid_point_tally / jnp.sqrt(jnp.maximum(predicted_spread_sum / grid_point_tally, minimum_divisor) * jnp.maximum(observed_dispersion / grid_point_tally, minimum_divisor))
    return (mean_square, average_error, covariance_sum)

def reference(prediction_fields, verifying_state, normal_state, evaluated_point_flag, parallels_each_strip):
    band_start = jnp.cumsum(parallels_each_strip) - parallels_each_strip
    slot_ids = jnp.arange(LAT_CAP, dtype=jnp.int32)
    global_row = (band_start[:, None] + slot_ids[None, :]).reshape(-1)
    inside_band = (slot_ids[None, :] < parallels_each_strip[:, None]).reshape(-1)
    angles = jnp.pi * jnp.arange(NLAT, dtype=jnp.float32) / (NLAT - 1)
    normalizer = jnp.sum(jnp.sin(angles))
    row_angle = jnp.pi * global_row.astype(jnp.float32) / (NLAT - 1)
    area_factors = jnp.where(inside_band, jnp.sin(row_angle) * NLAT / normalizer, 0.0).astype(jnp.float32)
    retain_filter = evaluated_point_flag.astype(jnp.float32) * inside_band.astype(jnp.float32)[None, :]
    observed_anomaly = verifying_state - normal_state
    observed_dispersion = lax.optimization_barrier(jnp.sum(retain_filter * observed_anomaly * observed_anomaly, axis=1))

    def by_horizon(predicted_step):
        predicted_anomaly = predicted_step - normal_state
        mistake_field = predicted_anomaly - observed_anomaly
        return (lax.optimization_barrier(jnp.sum(retain_filter * mistake_field * mistake_field, axis=1)), lax.optimization_barrier(jnp.sum(retain_filter * mistake_field, axis=1)), lax.optimization_barrier(jnp.sum(retain_filter * predicted_anomaly * observed_anomaly, axis=1)), lax.optimization_barrier(jnp.sum(retain_filter * predicted_anomaly * predicted_anomaly, axis=1)))
    error_power_two, prediction_error, paired_anomaly_term, predicted_spread_sum = lax.map(by_horizon, prediction_fields)
    parallel_quadratic_error, parallel_systematic_error, parallel_pattern_skill = final_result(error_power_two, prediction_error, paired_anomaly_term, predicted_spread_sum, observed_dispersion[None], EAST_WEST_SIZE)
    grid_points = NLAT * EAST_WEST_SIZE
    quadratic_error_total, systematic_error, pattern_skill = final_result(lax.optimization_barrier(jnp.sum(error_power_two * area_factors, axis=-1)), lax.optimization_barrier(jnp.sum(prediction_error * area_factors, axis=-1)), lax.optimization_barrier(jnp.sum(paired_anomaly_term * area_factors, axis=-1)), lax.optimization_barrier(jnp.sum(predicted_spread_sum * area_factors, axis=-1)), lax.optimization_barrier(jnp.sum(observed_dispersion * area_factors, axis=-1))[None], grid_points)
    rmse = jnp.sqrt(jnp.maximum(quadratic_error_total, minimum_divisor))
    return (parallel_quadratic_error, parallel_systematic_error, parallel_pattern_skill, rmse, systematic_error, pattern_skill)
```

```python
import functools
import math

import jax
import jax.numpy as jnp
import numpy as np
from jax import lax
from jax.experimental import pallas as pl
from jax.experimental.pallas import tpu as pltpu
from jax.sharding import PartitionSpec as P

MEAN_ROWS = 90
FLOOR = 0.1
SUB = 8


def up(n, m):
    return -(-n // m) * m


class Plan:
    def __init__(self, leads, nvar, nlon, width, lats, lons):
        self.leads, self.nvar, self.nlon, self.width = leads, nvar, nlon, width
        self.lats, self.lons = lats, lons
        self.lat_total = MEAN_ROWS * lats + 1
        self.lon_total = nlon * lons
        self.groups = nvar // SUB
        self.extra = nvar - self.groups * SUB
        self.quad = 4
        self.sums = 4 * leads + 1
        self.part = self.groups * SUB // self.quad
        self.slots = -(-SUB // self.quad)
        self.xrow = self.sums * self.part
        self.rrows = up(self.xrow + self.sums * self.slots, SUB)
        self.prow = self.part * leads
        self.grow0 = 3 * self.prow
        self.grow1 = self.grow0 + 3 * self.slots * leads
        self.gsum = up(self.sums, SUB)
        self.grows = self.grow1 + self.gsum

    def fits(self):
        return (
            self.lons == 2 * self.quad
            and self.groups % self.quad == 0
            and self.extra > 0
            and self.groups > 0
            and self.leads == 4
            and self.width == 128
            and self.grow1 % SUB == 0
        )


def sums_kernel(pn, pred, truth, norm, flag, rows, *refs):
    msgs, gout = refs[:4], refs[4]
    vp, vt, vn, vf, sp, keep, acc, sem = refs[5:]
    nl, w, lv = pn.nlon, pn.width, pn.leads
    per = nl * lv
    copies = [
        pltpu.make_async_copy(rows, sp, sem.at[0]),
        pltpu.make_async_copy(flag, vf, sem.at[1]),
        pltpu.make_async_copy(norm, vn, sem.at[2]),
        pltpu.make_async_copy(truth, vt, sem.at[3]),
    ]
    ng = pn.groups + 1
    for g in range(ng):
        n = SUB if g < pn.groups else pn.extra
        copies.append(
            pltpu.make_async_copy(
                pred.at[pl.ds(SUB * g, n)], vp.at[pl.ds(SUB * g, n)], sem.at[4 + g]
            )
        )
    for c in copies:
        c.start()
    me_lat = lax.axis_index("lat")
    quarter = lax.rem(lax.axis_index("lon"), pn.quad)
    copies[0].wait()
    first = jnp.int32(0)
    for b in range(pn.lats):
        first = first + jnp.where(b < me_lat, sp[b], 0)
    count = sp[me_lat]
    slot = lax.broadcasted_iota(jnp.int32, (SUB, w), 1)
    inside = slot < count
    row = first + slot
    fold = jnp.minimum(row, pn.lat_total - 1 - row).astype(jnp.float32)
    x = fold * np.float32(math.pi / (pn.lat_total - 1))
    x2 = x * x
    poly = jnp.full_like(x, 1.0 / math.factorial(13))
    for d in (11, 9, 7, 5, 3, 1):
        poly = poly * x2 * (-1.0) + 1.0 / math.factorial(d)
    total = float(np.sum(np.sin(np.pi * np.arange(pn.lat_total) / (pn.lat_total - 1))))
    weight = jnp.where(inside, poly * x * np.float32(pn.lat_total / total), 0.0)
    copies[1].wait()
    keep[...] = jnp.where(inside[0:1], vf[...], 0).astype(jnp.float32)
    copies[2].wait()
    copies[3].wait()
    flat = vp.reshape(pn.nvar * per, w)
    for g in range(ng):
        n = SUB if g < pn.groups else pn.extra
        copies[4 + g].wait()
        zero = jnp.zeros((n, w), jnp.float32)

        def body(l, c, g=g, n=n):
            k = keep[pl.ds(l, n, stride=0), :]
            a = vn[l, pl.ds(SUB * g, n), :]
            t = (vt[l, pl.ds(SUB * g, n), :] - a) * k
            a = a * k
            out = []
            for q in range(lv):
                f = flat[pl.ds(SUB * g * per + l * lv + q, n, stride=per), :] * k - a
                e = f - t
                out.append((c[q] + e * e, c[lv + q] + e, c[2 * lv + q] + f * t, c[3 * lv + q] + f * f))
            return tuple(out[q][m] for m in range(4) for q in range(lv)) + (c[4 * lv] + t * t,)

        c = lax.fori_loop(0, nl, body, (zero,) * pn.sums, unroll=3)
        for j in range(pn.sums):
            acc[j, pl.ds(SUB * g, n), :] = c[j]
    top = SUB * pn.groups
    for j in range(pn.sums):
        acc[j, pl.ds(top + pn.extra, SUB - pn.extra), :] = jnp.zeros((SUB - pn.extra, w), jnp.float32)
    for k in range(pn.quad):
        p = quarter ^ k
        for j in range(pn.sums):
            base = pl.multiple_of(p * pn.part, SUB)
            msgs[k][pl.ds(j * pn.part, pn.part), :] = acc[j, pl.ds(base, pn.part), :]
            msgs[k][pl.ds(pn.xrow + j * pn.slots, pn.slots), :] = acc[
                j, pl.ds(top + p, pn.slots, stride=pn.quad), :
            ]
        used = pn.xrow + pn.sums * pn.slots
        msgs[k][pl.ds(used, pn.rrows - used), :] = jnp.zeros((pn.rrows - used, w), jnp.float32)
    gout[...] = jnp.zeros((pn.gsum, w), jnp.float32)
    for j in range(pn.sums):
        d = lax.dot_general(
            weight,
            acc[j],
            (((1,), (1,)), ((), ())),
            precision=lax.Precision.HIGHEST,
            preferred_element_type=jnp.float32,
        )
        gout[pl.ds(j, 1), pl.ds(0, top + SUB)] = d[0:1]


def add_kernel(pn, own, r1, r2, r3, g, out):
    out[pl.ds(0, pn.rrows), :] = (own[...] + r1[...]) + (r2[...] + r3[...])
    out[pl.ds(pn.rrows, pn.gsum), :] = g[...]


def metrics(sq, off, pr, sp, tt, n):
    skill = (pr / n) / jnp.sqrt(jnp.maximum(sp / n, FLOOR) * jnp.maximum(tt / n, FLOOR))
    return sq / n, off / n, skill


def final_kernel(pn, own, far, out):
    n = np.float32(pn.lon_total)
    lv = pn.leads

    def rows(r, m):
        return own[pl.ds(r, m), :] + far[pl.ds(r, m), :]

    tt = rows(4 * lv * pn.part, pn.part)
    for q in range(lv):
        vals = metrics(*(rows((m * lv + q) * pn.part, pn.part) for m in range(4)), tt, n)
        for i in range(3):
            out[pl.ds(i * pn.prow + q, pn.part, stride=lv), :] = vals[i]
    x = pn.xrow
    tt = rows(x + 4 * lv * pn.slots, pn.slots)
    for q in range(lv):
        vals = metrics(*(rows(x + (m * lv + q) * pn.slots, pn.slots) for m in range(4)), tt, n)
        for i in range(3):
            out[pl.ds(pn.grow0 + i * pn.slots * lv + q, pn.slots, stride=lv), :] = vals[i]
    out[pl.ds(pn.grow1, pn.gsum), :] = rows(pn.rrows, pn.gsum)


def place_kernel(pn, own, r1, r2, r3, *outs):
    lv = pn.leads
    quarter = lax.rem(lax.axis_index("lon"), pn.quad)
    got = (own, r1, r2, r3)
    top = SUB * pn.groups * lv
    flats = [outs[i].reshape(pn.nvar * lv, pn.width) for i in range(3)]
    for k in range(pn.quad):
        p = quarter ^ k
        for i in range(3):
            flats[i][pl.ds(pl.multiple_of(p * pn.prow, SUB), pn.prow), :] = got[k][pl.ds(i * pn.prow, pn.prow), :]
            for s in range(pn.slots):
                @pl.when(p + s * pn.quad < pn.extra)
                def _(i=i, s=s, k=k, p=p):
                    outs[i][SUB * pn.groups + p + s * pn.quad] = got[k][
                        pl.ds(pn.grow0 + (i * pn.slots + s) * lv, lv), :
                    ]
    a, b, c, d = (r[pl.ds(pn.grow1, pn.gsum), :] for r in got)
    g = (a + b) + (c + d)
    n = np.float32(pn.lat_total * pn.lon_total)
    mse, off, skill = metrics(*(g[m * lv:(m + 1) * lv] for m in range(4)), g[4 * lv:4 * lv + 1], n)
    outs[3][...] = jnp.sqrt(jnp.maximum(mse, FLOOR))[:, : pn.nvar]
    outs[4][...] = off[:, : pn.nvar]
    outs[5][...] = skill[:, : pn.nvar]


def fast(pn, pred, truth, norm, flag, rows):
    f32 = jnp.float32
    w, lv = pn.width, pn.leads
    vm = pl.BlockSpec(memory_space=pltpu.VMEM)
    hbm = pl.BlockSpec(memory_space=pltpu.HBM)
    pred = jnp.transpose(pred, (1, 2, 0, 3))
    truth = jnp.transpose(truth, (1, 0, 2))
    norm = jnp.transpose(norm, (1, 0, 2))
    limit = pltpu.CompilerParams(vmem_limit_bytes=63 * 2**20)
    small = pltpu.CompilerParams(vmem_limit_bytes=8 * 2**20)
    rmsg = jax.ShapeDtypeStruct((pn.rrows, w), f32)
    gmsg = jax.ShapeDtypeStruct((pn.gsum, w), f32)
    *msgs, g = pl.pallas_call(
        functools.partial(sums_kernel, pn),
        out_shape=[rmsg] * 4 + [gmsg],
        in_specs=[hbm] * 5,
        out_specs=[vm] * 5,
        scratch_shapes=[
            pltpu.VMEM(pred.shape, f32),
            pltpu.VMEM(truth.shape, f32),
            pltpu.VMEM(norm.shape, f32),
            pltpu.VMEM(flag.shape, jnp.int32),
            pltpu.SMEM(rows.shape, jnp.int32),
            pltpu.VMEM(flag.shape, f32),
            pltpu.VMEM((pn.sums, SUB * (pn.groups + 1), w), f32),
            pltpu.SemaphoreType.DMA((5 + pn.groups,)),
        ],
        compiler_params=limit,
        name="sums",
    )(pred, truth, norm, flag, rows)

    def swap(x, k):
        return lax.ppermute(x, "lon", [(i, i ^ k) for i in range(pn.lons)])

    near = [swap(msgs[k], k) for k in (3, 1, 2)]
    step = 1
    while step < pn.lats:
        g = g + lax.ppermute(g, "lat", [(i, i ^ step) for i in range(pn.lats)])
        step *= 2
    smsg = jax.ShapeDtypeStruct((pn.rrows + pn.gsum, w), f32)
    part = pl.pallas_call(
        functools.partial(add_kernel, pn), out_shape=smsg, in_specs=[vm] * 5, out_specs=vm, compiler_params=small, name="near_add"
    )(msgs[0], *near, g)
    far = swap(part, pn.quad)
    done = pl.pallas_call(
        functools.partial(final_kernel, pn),
        out_shape=jax.ShapeDtypeStruct((pn.grows, w), f32),
        in_specs=[vm] * 2,
        out_specs=vm,
        compiler_params=small,
        name="metrics",
    )(part, far)
    got = {k: swap(done, k) for k in (3, 1, 2)}
    outs = pl.pallas_call(
        functools.partial(place_kernel, pn),
        out_shape=[jax.ShapeDtypeStruct((pn.nvar, lv, w), f32)] * 3
        + [jax.ShapeDtypeStruct((lv, pn.nvar), f32)] * 3,
        in_specs=[vm] * 4,
        compiler_params=small,
        name="place",
    )(done, got[1], got[2], got[3])
    return tuple(jnp.transpose(o, (1, 0, 2)) for o in outs[:3]) + tuple(outs[3:])


def plain(pn, pred, truth, norm, flag, rows):
    band = lax.axis_index("lat")
    ids = jnp.arange(pn.lats, dtype=jnp.int32)
    first = jnp.sum(jnp.where(ids < band, rows, 0))
    count = jnp.sum(jnp.where(ids == band, rows, 0))
    slot = jnp.arange(pn.width, dtype=jnp.int32)
    inside = slot < count
    angles = jnp.pi * jnp.arange(pn.lat_total, dtype=jnp.float32) / (pn.lat_total - 1)
    angle = jnp.pi * (first + slot).astype(jnp.float32) / (pn.lat_total - 1)
    weight = jnp.where(inside, jnp.sin(angle) * pn.lat_total / jnp.sum(jnp.sin(angles)), 0.0)
    keep = flag.astype(jnp.float32) * inside.astype(jnp.float32)[None, :]
    t = truth - norm
    f = pred - norm[None]
    e = f - t[None]
    k = keep[None, None]
    sums = jnp.concatenate(
        [
            jnp.sum(k * e * e, axis=2),
            jnp.sum(k * e, axis=2),
            jnp.sum(k * f * t[None], axis=2),
            jnp.sum(k * f * f, axis=2),
            jnp.sum(k * t[None] * t[None], axis=2),
        ],
        axis=0,
    )
    grand = lax.psum(jnp.sum(sums * weight, axis=2), ("lat", "lon"))
    zonal = lax.psum(sums, "lon")

    def finish(s, n):
        parts = [s[m * pn.leads:(m + 1) * pn.leads] for m in range(4)]
        return metrics(*parts, s[4 * pn.leads:], n)

    mse, off, skill = finish(zonal, float(pn.lon_total))
    gm, go, gs = finish(grand, float(pn.lat_total * pn.lon_total))
    return mse, off, skill, jnp.sqrt(jnp.maximum(gm, FLOOR)), go, gs


def local(pred, truth, norm, flag, rows):
    leads, nvar, nlon, width = pred.shape
    pn = Plan(leads, nvar, nlon, width, lax.axis_size("lat"), lax.axis_size("lon"))
    return (fast if pn.fits() else plain)(pn, pred, truth, norm, flag, rows)


def solution(mesh):
    in_specs = (
        P(None, None, "lon", "lat"),
        P(None, "lon", "lat"),
        P(None, "lon", "lat"),
        P("lon", "lat"),
        P(),
    )
    out_specs = (P(None, None, "lat"), P(None, None, "lat"), P(None, None, "lat"), P(), P(), P())
    return jax.shard_map(local, mesh=mesh, in_specs=in_specs, out_specs=out_specs, check_vma=False)
```

```python
import functools
import math

import jax
import jax.numpy as jnp
import numpy as np
from jax import lax
from jax.experimental import pallas as pl
from jax.experimental.pallas import tpu as pltpu
from jax.sharding import PartitionSpec as P


MEAN_ROWS = 90
FLOOR = 0.1
SUB = 8
UNROLL = 9
NEAR = (1, 3, 2)
BACK = (3, 1, 2)


def up(n, m):
    return -(-n // m) * m


class Plan:
    def __init__(self, leads, nvar, nlon, width, lats, lons):
        self.leads, self.nvar, self.nlon, self.width = leads, nvar, nlon, width
        self.lats, self.lons = lats, lons
        self.lat_total = MEAN_ROWS * lats + 1
        self.lon_total = nlon * lons
        self.quad = 4
        self.groups = nvar // SUB
        self.chunks = self.groups // self.quad
        self.top = self.groups * SUB
        self.extra = nvar - self.top
        self.sums = 4 * leads + 1
        self.slots = SUB // self.quad
        self.gsum = up(self.sums, SUB)
        self.xrow = self.sums * SUB
        self.rrows = [self.xrow] * (self.chunks - 1) + [up(self.xrow + self.sums * self.slots, SUB)]
        self.prow = SUB * leads
        self.grow0 = 3 * self.prow
        self.grows = [self.grow0 + self.gsum] * (self.chunks - 1) + [self.grow0 + 3 * self.slots * leads]

    def last(self, c):
        return c == self.chunks - 1

    def fits(self):
        return (
            self.lons == 2 * self.quad
            and self.chunks == 2
            and self.groups == self.chunks * self.quad
            and self.extra > 0
            and self.leads == 4
            and self.width == 128
        )


def sums_kernel(pn, pred, truth, norm, flag, rows, *refs):
    msgs = refs[:pn.quad]
    acc, wout, vp, vt, vn, vf, sp, keep, sem = refs[pn.quad:]
    w, lv = pn.width, pn.leads
    per = pn.nlon * lv
    starts = [SUB * g for g in range(pn.groups)] + [pn.top]
    sizes = [SUB] * pn.groups + [pn.extra]
    copies = [
        pltpu.make_async_copy(rows, sp, sem.at[0]),
        pltpu.make_async_copy(flag, vf, sem.at[1]),
    ]
    for i, (v, n) in enumerate(zip(starts, sizes)):
        copies += [
            pltpu.make_async_copy(norm.at[:, pl.ds(v, n)], vn.at[:, pl.ds(v, n)], sem.at[3 * i + 2]),
            pltpu.make_async_copy(truth.at[:, pl.ds(v, n)], vt.at[:, pl.ds(v, n)], sem.at[3 * i + 3]),
            pltpu.make_async_copy(pred.at[pl.ds(v, n)], vp.at[pl.ds(v, n)], sem.at[3 * i + 4]),
        ]
    for c in copies:
        c.start()
    for j in range(pn.sums):
        acc[j, pl.ds(pn.top, SUB), :] = jnp.zeros((SUB, w), jnp.float32)
    me_lat = lax.axis_index("lat")
    quarter = lax.rem(lax.axis_index("lon"), pn.quad)
    copies[0].wait()
    first = jnp.int32(0)
    for b in range(pn.lats):
        first = first + jnp.where(b < me_lat, sp[b], 0)
    slot = lax.broadcasted_iota(jnp.int32, (SUB, w), 1)
    inside = slot < sp[me_lat]
    row = first + slot
    fold = jnp.minimum(row, pn.lat_total - 1 - row).astype(jnp.float32)
    x = fold * np.float32(math.pi / (pn.lat_total - 1))
    x2 = x * x
    poly = jnp.full_like(x, 1.0 / math.factorial(13))
    for d in (11, 9, 7, 5, 3, 1):
        poly = poly * x2 * (-1.0) + 1.0 / math.factorial(d)
    total = float(np.sum(np.sin(np.pi * np.arange(pn.lat_total) / (pn.lat_total - 1))))
    wout[...] = jnp.where(inside, poly * x * np.float32(pn.lat_total / total), 0.0)
    copies[1].wait()
    keep[...] = jnp.where(inside[0:1], vf[...], 0).astype(jnp.float32)
    flat = vp.reshape(pn.nvar * per, w)
    for i, (v, n) in enumerate(zip(starts, sizes)):
        for c in copies[3 * i + 2:3 * i + 5]:
            c.wait()
        zero = jnp.zeros((n, w), jnp.float32)

        def body(l, c, v=v, n=n):
            k = keep[pl.ds(l, n, stride=0), :]
            a = vn[l, pl.ds(v, n), :]
            t = (vt[l, pl.ds(v, n), :] - a) * k
            a = a * k
            out = []
            for q in range(lv):
                f = flat[pl.ds(v * per + l * lv + q, n, stride=per), :] * k - a
                e = f - t
                out.append((c[q] + e * e, c[lv + q] + e, c[2 * lv + q] + f * t, c[3 * lv + q] + f * f))
            return tuple(out[q][m] for m in range(4) for q in range(lv)) + (c[4 * lv] + t * t,)

        c = lax.fori_loop(0, pn.nlon, body, (zero,) * pn.sums, unroll=UNROLL)
        for j in range(pn.sums):
            acc[j, pl.ds(v, n), :] = c[j]
    for c in range(pn.chunks):
        for k in range(pn.quad):
            p = quarter ^ k
            base = pl.multiple_of(SUB * (pn.chunks * p + c), SUB)
            at = sum(pn.rrows[:c])
            for j in range(pn.sums):
                msgs[k][pl.ds(at + j * SUB, SUB), :] = acc[j, pl.ds(base, SUB), :]
            if pn.last(c):
                for j in range(pn.sums):
                    msgs[k][pl.ds(at + pn.xrow + j * pn.slots, pn.slots), :] = acc[
                        j, pl.ds(pn.top + p, pn.slots, stride=pn.quad), :
                    ]
                used = pn.xrow + pn.sums * pn.slots
                if used < pn.rrows[c]:
                    msgs[k][pl.ds(at + used, pn.rrows[c] - used), :] = jnp.zeros((pn.rrows[c] - used, w), jnp.float32)


def weigh_kernel(pn, wt, acc, gout):
    gout[...] = jnp.zeros((pn.gsum, pn.width), jnp.float32)
    for j in range(pn.sums):
        d = lax.dot_general(
            wt[...],
            acc[j],
            (((1,), (1,)), ((), ())),
            precision=lax.Precision.HIGHEST,
            preferred_element_type=jnp.float32,
        )
        gout[pl.ds(j, 1), pl.ds(0, pn.top + SUB)] = d[0:1]


def add_kernel(pn, own, r1, r2, r3, g, out):
    n = sum(pn.rrows)
    out[pl.ds(0, n), :] = (own[...] + r1[...]) + (r2[...] + r3[...])
    out[pl.ds(n, pn.gsum), :] = g[...]


def metrics(sq, off, pr, sp, tt, n):
    skill = (pr / n) / jnp.sqrt(jnp.maximum(sp / n, FLOOR) * jnp.maximum(tt / n, FLOOR))
    return sq / n, off / n, skill


def final_kernel(pn, own, far, out):
    n = np.float32(pn.lon_total)
    lv = pn.leads

    def rows(r, m):
        return own[pl.ds(r, m), :] + far[pl.ds(r, m), :]

    for c in range(pn.chunks):
        at, to = sum(pn.rrows[:c]), sum(pn.grows[:c])
        parts = [(0, SUB, 0)]
        if pn.last(c):
            parts.append((pn.xrow, pn.slots, pn.grow0))
        for x, m, y in parts:
            tt = rows(at + x + 4 * lv * m, m)
            for q in range(lv):
                vals = metrics(*(rows(at + x + (d * lv + q) * m, m) for d in range(4)), tt, n)
                for i in range(3):
                    out[pl.ds(to + y + i * m * lv + q, m, stride=lv), :] = vals[i]
    out[pl.ds(pn.grow0, pn.gsum), :] = rows(sum(pn.rrows), pn.gsum)


def place_kernel(pn, *refs):
    lv = pn.leads
    quarter = lax.rem(lax.axis_index("lon"), pn.quad)
    base = refs[:pn.quad]
    got = [[r.at[pl.ds(sum(pn.grows[:c]), pn.grows[c])] for r in base] for c in range(pn.chunks)]
    outs = refs[pn.quad:]
    flats = [outs[i].reshape(pn.nvar * lv, pn.width) for i in range(3)]
    for k in range(pn.quad):
        p = quarter ^ k
        for i in range(3):
            for c in range(pn.chunks):
                base = pl.multiple_of((pn.chunks * p + c) * pn.prow, SUB)
                flats[i][pl.ds(base, pn.prow), :] = got[c][k][pl.ds(i * pn.prow, pn.prow), :]
            for s in range(pn.slots):
                @pl.when(p + s * pn.quad < pn.extra)
                def _(i=i, s=s, k=k, p=p):
                    outs[i][pn.top + p + s * pn.quad] = got[-1][k][
                        pl.ds(pn.grow0 + (i * pn.slots + s) * lv, lv), :
                    ]
    a, b, c, d = (r[pl.ds(pn.grow0, pn.gsum), :] for r in got[0])
    g = (a + b) + (c + d)
    n = np.float32(pn.lat_total * pn.lon_total)
    mse, off, skill = metrics(*(g[m * lv:(m + 1) * lv] for m in range(4)), g[4 * lv:4 * lv + 1], n)
    outs[3][...] = jnp.sqrt(jnp.maximum(mse, FLOOR))[:, : pn.nvar]
    outs[4][...] = off[:, : pn.nvar]
    outs[5][...] = skill[:, : pn.nvar]


def fast(pn, pred, truth, norm, flag, rows):
    f32 = jnp.float32
    w, lv = pn.width, pn.leads
    vm = pl.BlockSpec(memory_space=pltpu.VMEM)
    hbm = pl.BlockSpec(memory_space=pltpu.HBM)
    pred = jnp.transpose(pred, (1, 2, 0, 3))
    truth = jnp.transpose(truth, (1, 0, 2))
    norm = jnp.transpose(norm, (1, 0, 2))
    large = pltpu.CompilerParams(vmem_limit_bytes=24 * 2**20)
    small = pltpu.CompilerParams(vmem_limit_bytes=8 * 2**20)

    def arr(*shape):
        return jax.ShapeDtypeStruct(shape, f32)

    def call(kernel, out, *args):
        return pl.pallas_call(
            kernel,
            out_shape=out,
            in_specs=[vm] * len(args),
            out_specs=jax.tree.map(lambda _: vm, out),
            compiler_params=small,
        )(*args)

    def swap(x, k):
        return lax.ppermute(x, "lon", [(i, i ^ k) for i in range(pn.lons)])

    inputs = [pltpu.with_memory_space_constraint(a, pltpu.HBM) for a in (pred, truth, norm, flag, rows)]
    *msgs, acc, wt = pl.pallas_call(
        functools.partial(sums_kernel, pn),
        out_shape=[arr(sum(pn.rrows), w)] * pn.quad
        + [arr(pn.sums, pn.top + SUB, w), arr(SUB, w)],
        in_specs=[hbm] * 5,
        out_specs=[vm] * (pn.quad + 2),
        scratch_shapes=[
            pltpu.VMEM(pred.shape, f32),
            pltpu.VMEM(truth.shape, f32),
            pltpu.VMEM(norm.shape, f32),
            pltpu.VMEM(flag.shape, jnp.int32),
            pltpu.SMEM(rows.shape, jnp.int32),
            pltpu.VMEM(flag.shape, f32),
            pltpu.SemaphoreType.DMA((2 + 3 * (pn.groups + 1),)),
        ],
        compiler_params=large,
        name="sums",
    )(*inputs)
    near = {k: swap(msgs[k], k) for k in NEAR}
    g = call(functools.partial(weigh_kernel, pn), arr(pn.gsum, w), wt, acc)
    step = 1
    while step < pn.lats:
        g = g + lax.ppermute(g, "lat", [(i, i ^ step) for i in range(pn.lats)])
        step *= 2
    part = call(
        functools.partial(add_kernel, pn), arr(sum(pn.rrows) + pn.gsum, w),
        msgs[0], near[1], near[2], near[3], g,
    )
    far = swap(part, pn.quad)
    done = call(functools.partial(final_kernel, pn), arr(sum(pn.grows), w), part, far)
    there = {k: swap(done, k) for k in BACK}
    got = [done, there[1], there[2], there[3]]
    outs = pl.pallas_call(
        functools.partial(place_kernel, pn),
        out_shape=[arr(pn.nvar, lv, w)] * 3 + [arr(lv, pn.nvar)] * 3,
        in_specs=[vm] * len(got),
        compiler_params=small,
        name="place",
    )(*got)
    return tuple(jnp.transpose(o, (1, 0, 2)) for o in outs[:3]) + tuple(outs[3:])


def plain(pn, pred, truth, norm, flag, rows):
    band = lax.axis_index("lat")
    ids = jnp.arange(pn.lats, dtype=jnp.int32)
    first = jnp.sum(jnp.where(ids < band, rows, 0))
    count = jnp.sum(jnp.where(ids == band, rows, 0))
    slot = jnp.arange(pn.width, dtype=jnp.int32)
    inside = slot < count
    angles = jnp.pi * jnp.arange(pn.lat_total, dtype=jnp.float32) / (pn.lat_total - 1)
    angle = jnp.pi * (first + slot).astype(jnp.float32) / (pn.lat_total - 1)
    weight = jnp.where(inside, jnp.sin(angle) * pn.lat_total / jnp.sum(jnp.sin(angles)), 0.0)
    keep = flag.astype(jnp.float32) * inside.astype(jnp.float32)[None, :]
    t = truth - norm
    f = pred - norm[None]
    e = f - t[None]
    k = keep[None, None]
    sums = jnp.concatenate(
        [
            jnp.sum(k * e * e, axis=2),
            jnp.sum(k * e, axis=2),
            jnp.sum(k * f * t[None], axis=2),
            jnp.sum(k * f * f, axis=2),
            jnp.sum(k * t[None] * t[None], axis=2),
        ],
        axis=0,
    )
    grand = lax.psum(jnp.sum(sums * weight, axis=2), ("lat", "lon"))
    zonal = lax.psum(sums, "lon")

    def finish(s, n):
        parts = [s[m * pn.leads:(m + 1) * pn.leads] for m in range(4)]
        return metrics(*parts, s[4 * pn.leads:], n)

    mse, off, skill = finish(zonal, float(pn.lon_total))
    gm, go, gs = finish(grand, float(pn.lat_total * pn.lon_total))
    return mse, off, skill, jnp.sqrt(jnp.maximum(gm, FLOOR)), go, gs


def local(pred, truth, norm, flag, rows):
    leads, nvar, nlon, width = pred.shape
    pn = Plan(leads, nvar, nlon, width, lax.axis_size("lat"), lax.axis_size("lon"))
    return (fast if pn.fits() else plain)(pn, pred, truth, norm, flag, rows)


def solution(mesh):
    in_specs = (
        P(None, None, "lon", "lat"),
        P(None, "lon", "lat"),
        P(None, "lon", "lat"),
        P("lon", "lat"),
        P(),
    )
    out_specs = (P(None, None, "lat"), P(None, None, "lat"), P(None, None, "lat"), P(), P(), P())
    return jax.shard_map(local, mesh=mesh, in_specs=in_specs, out_specs=out_specs, check_vma=False)
```

```python
import functools
import math

import jax
import jax.numpy as jnp
import numpy as np
from jax import lax
from jax.experimental import pallas as pl
from jax.experimental.pallas import tpu as pltpu
from jax.sharding import PartitionSpec as P


MEAN_ROWS = 90
FLOOR = 0.1
SUB = 8
UNROLL = 9
PIECES = 3
NEAR = (1, 3, 2)
BACK = (3, 1, 2)


class Plan:
    def __init__(self, leads, nvar, nlon, width, lats, lons):
        self.leads, self.nvar, self.nlon, self.width = leads, nvar, nlon, width
        self.lats, self.lons = lats, lons
        self.lat_total = MEAN_ROWS * lats + 1
        self.lon_total = nlon * lons
        self.quad = 4
        self.groups = nvar // SUB
        self.chunks = self.groups // self.quad
        self.top = self.groups * SUB
        self.extra = nvar - self.top
        self.sums = 4 * leads + 1
        self.xrow = self.sums * SUB
        self.rrows = self.chunks * self.xrow + 5 * self.extra
        self.prow = SUB * leads
        self.grow0 = self.chunks * 3 * self.prow
        self.grow1 = self.grow0 + 3 * self.extra

    def fits(self):
        return (
            self.lons == 2 * self.quad
            and self.chunks == 2
            and self.groups == self.chunks * self.quad
            and self.extra > 0
            and self.leads == self.quad
            and self.width == 128
        )


def sums_kernel(pn, pred, truth, norm, flag, rows, *refs):
    msgs = refs[:pn.quad]
    acc, wout, vp, vt, vn, vf, sp, keep, sem = refs[pn.quad:]
    w, lv = pn.width, pn.leads
    per = pn.nlon * lv
    groups = [(pn.top, pn.extra)] + [(SUB * g, SUB) for g in range(pn.groups)]
    cuts = [pn.nlon * i // PIECES for i in range(PIECES + 1)]
    pieces = [(v, n, 0, pn.nlon) for v, n in groups[:-1]]
    pieces += [groups[-1] + (lo, hi) for lo, hi in zip(cuts, cuts[1:])]
    copies = [
        pltpu.make_async_copy(rows, sp, sem.at[0]),
        pltpu.make_async_copy(flag, vf, sem.at[1]),
    ]
    for i, (v, n, lo, hi) in enumerate(pieces):
        var, lon = pl.ds(v, n), pl.ds(lo, hi - lo)
        copies += [
            pltpu.make_async_copy(norm.at[lon, var], vn.at[lon, var], sem.at[3 * i + 2]),
            pltpu.make_async_copy(truth.at[lon, var], vt.at[lon, var], sem.at[3 * i + 3]),
            pltpu.make_async_copy(pred.at[var, lon], vp.at[var, lon], sem.at[3 * i + 4]),
        ]
    for c in copies:
        c.start()
    for j in range(pn.sums):
        acc[j, pl.ds(pn.top, SUB), :] = jnp.zeros((SUB, w), jnp.float32)
    me_lat = lax.axis_index("lat")
    quarter = lax.rem(lax.axis_index("lon"), pn.quad)
    copies[0].wait()
    first = jnp.int32(0)
    for b in range(pn.lats):
        first = first + jnp.where(b < me_lat, sp[b], 0)
    slot = lax.broadcasted_iota(jnp.int32, (SUB, w), 1)
    inside = slot < sp[me_lat]
    row = first + slot
    fold = jnp.minimum(row, pn.lat_total - 1 - row).astype(jnp.float32)
    x = fold * np.float32(math.pi / (pn.lat_total - 1))
    x2 = x * x
    poly = jnp.full_like(x, 1.0 / math.factorial(13))
    for d in (11, 9, 7, 5, 3, 1):
        poly = poly * x2 * (-1.0) + 1.0 / math.factorial(d)
    norms = float(np.sum(np.sin(np.pi * np.arange(pn.lat_total) / (pn.lat_total - 1))))
    wout[...] = jnp.where(inside, poly * x * np.float32(pn.lat_total / norms), 0.0)
    copies[1].wait()
    keep[...] = jnp.where(inside[0:1], vf[...], 0).astype(jnp.float32)
    flat = vp.reshape(pn.nvar * per, w)
    for i, (v, n, lo, hi) in enumerate(pieces):
        for c in copies[3 * i + 2:3 * i + 5]:
            c.wait()

        def body(l, c, v=v, n=n):
            k = keep[pl.ds(l, n, stride=0), :]
            a = vn[l, pl.ds(v, n), :]
            t = (vt[l, pl.ds(v, n), :] - a) * k
            a = a * k
            out = []
            for q in range(lv):
                f = flat[pl.ds(v * per + l * lv + q, n, stride=per), :] * k - a
                e = f - t
                out.append((c[q] + e * e, c[lv + q] + e, c[2 * lv + q] + f * t, c[3 * lv + q] + f * f))
            return tuple(out[q][m] for m in range(4) for q in range(lv)) + (c[4 * lv] + t * t,)

        if lo == 0:
            total = (jnp.zeros((n, w), jnp.float32),) * pn.sums
        total = lax.fori_loop(lo, hi, body, total, unroll=UNROLL if hi - lo == pn.nlon else hi - lo)
        if hi == pn.nlon:
            for j in range(pn.sums):
                acc[j, pl.ds(v, n), :] = total[j]
    for c in range(pn.chunks):
        for k in range(pn.quad):
            p = quarter ^ k
            base = pl.multiple_of(SUB * (pn.chunks * p + c), SUB)
            for j in range(pn.sums):
                msgs[k][pl.ds(c * pn.xrow + j * SUB, SUB), :] = acc[j, pl.ds(base, SUB), :]
    for k in range(pn.quad):
        p = quarter ^ k
        for m in range(5):
            j = m * lv + (p if m < 4 else 0)
            msgs[k][pl.ds(pn.chunks * pn.xrow + m * pn.extra, pn.extra), :] = acc[j, pl.ds(pn.top, pn.extra), :]


def weigh_kernel(pn, wt, acc, gout):
    gout[...] = jnp.zeros((pn.sums, pn.width), jnp.float32)
    for j in range(pn.sums):
        d = lax.dot_general(
            wt[...],
            acc[j],
            (((1,), (1,)), ((), ())),
            precision=lax.Precision.HIGHEST,
            preferred_element_type=jnp.float32,
        )
        gout[pl.ds(j, 1), pl.ds(0, pn.top + SUB)] = d[0:1]


def add_kernel(pn, own, r1, r2, r3, g, out):
    out[pl.ds(0, pn.rrows), :] = (own[...] + r1[...]) + (r2[...] + r3[...])
    out[pl.ds(pn.rrows, pn.sums), :] = g[...]


def metrics(sq, off, pr, sp, tt, n):
    skill = (pr / n) / jnp.sqrt(jnp.maximum(sp / n, FLOOR) * jnp.maximum(tt / n, FLOOR))
    return sq / n, off / n, skill


def final_kernel(pn, own, far, out):
    n = np.float32(pn.lon_total)
    lv = pn.leads

    def rows(r, m):
        return own[pl.ds(r, m), :] + far[pl.ds(r, m), :]

    for c in range(pn.chunks):
        at, to = c * pn.xrow, c * 3 * pn.prow
        tt = rows(at + 4 * lv * SUB, SUB)
        for q in range(lv):
            vals = metrics(*(rows(at + (d * lv + q) * SUB, SUB) for d in range(4)), tt, n)
            for i in range(3):
                out[pl.ds(to + i * pn.prow + q, SUB, stride=lv), :] = vals[i]
    x = pn.chunks * pn.xrow
    vals = metrics(*(rows(x + m * pn.extra, pn.extra) for m in range(5)), n)
    for i in range(3):
        out[pl.ds(pn.grow0 + i * pn.extra, pn.extra), :] = vals[i]
    out[pl.ds(pn.grow1, pn.sums), :] = rows(pn.rrows, pn.sums)


def place_kernel(pn, *refs):
    lv = pn.leads
    quarter = lax.rem(lax.axis_index("lon"), pn.quad)
    got, outs = refs[:pn.quad], refs[pn.quad:]
    flats = [outs[i].reshape(pn.nvar * lv, pn.width) for i in range(3)]
    for k in range(pn.quad):
        p = quarter ^ k
        for i in range(3):
            for c in range(pn.chunks):
                base = pl.multiple_of((pn.chunks * p + c) * pn.prow, SUB)
                flats[i][pl.ds(base, pn.prow), :] = got[k][pl.ds((3 * c + i) * pn.prow, pn.prow), :]
            flats[i][pl.ds(pn.top * lv + p, pn.extra, stride=lv), :] = got[k][
                pl.ds(pn.grow0 + i * pn.extra, pn.extra), :
            ]
    a, b, c, d = (r[pl.ds(pn.grow1, pn.sums), :] for r in got)
    g = (a + b) + (c + d)
    n = np.float32(pn.lat_total * pn.lon_total)
    mse, off, skill = metrics(*(g[m * lv:(m + 1) * lv] for m in range(4)), g[4 * lv:4 * lv + 1], n)
    outs[3][...] = jnp.sqrt(jnp.maximum(mse, FLOOR))[:, : pn.nvar]
    outs[4][...] = off[:, : pn.nvar]
    outs[5][...] = skill[:, : pn.nvar]


def fast(pn, pred, truth, norm, flag, rows):
    f32 = jnp.float32
    w, lv = pn.width, pn.leads
    vm = pl.BlockSpec(memory_space=pltpu.VMEM)
    hbm = pl.BlockSpec(memory_space=pltpu.HBM)
    pred = jnp.transpose(pred, (1, 2, 0, 3))
    truth = jnp.transpose(truth, (1, 0, 2))
    norm = jnp.transpose(norm, (1, 0, 2))
    large = pltpu.CompilerParams(vmem_limit_bytes=24 * 2**20)
    small = pltpu.CompilerParams(vmem_limit_bytes=8 * 2**20)

    def arr(*shape):
        return jax.ShapeDtypeStruct(shape, f32)

    def call(kernel, out, *args):
        return pl.pallas_call(
            kernel,
            out_shape=out,
            in_specs=[vm] * len(args),
            out_specs=jax.tree.map(lambda _: vm, out),
            compiler_params=small,
        )(*args)

    def swap(x, k):
        return lax.ppermute(x, "lon", [(i, i ^ k) for i in range(pn.lons)])

    inputs = [pltpu.with_memory_space_constraint(a, pltpu.HBM) for a in (pred, truth, norm, flag, rows)]
    *msgs, acc, wt = pl.pallas_call(
        functools.partial(sums_kernel, pn),
        out_shape=[arr(pn.rrows, w)] * pn.quad
        + [arr(pn.sums, pn.top + SUB, w), arr(SUB, w)],
        in_specs=[hbm] * 5,
        out_specs=[vm] * (pn.quad + 2),
        scratch_shapes=[
            pltpu.VMEM(pred.shape, f32),
            pltpu.VMEM(truth.shape, f32),
            pltpu.VMEM(norm.shape, f32),
            pltpu.VMEM(flag.shape, jnp.int32),
            pltpu.SMEM(rows.shape, jnp.int32),
            pltpu.VMEM(flag.shape, f32),
            pltpu.SemaphoreType.DMA((2 + 3 * (pn.groups + PIECES),)),
        ],
        compiler_params=large,
        name="sums",
    )(*inputs)
    near = {k: swap(msgs[k], k) for k in NEAR}
    g = call(functools.partial(weigh_kernel, pn), arr(pn.sums, w), wt, acc)
    step = 1
    while step < pn.lats:
        g = g + lax.ppermute(g, "lat", [(i, i ^ step) for i in range(pn.lats)])
        step *= 2
    part = call(
        functools.partial(add_kernel, pn), arr(pn.rrows + pn.sums, w),
        msgs[0], near[1], near[2], near[3], g,
    )
    far = swap(part, pn.quad)
    done = call(functools.partial(final_kernel, pn), arr(pn.grow1 + pn.sums, w), part, far)
    there = {k: swap(done, k) for k in BACK}
    got = [done, there[1], there[2], there[3]]
    outs = pl.pallas_call(
        functools.partial(place_kernel, pn),
        out_shape=[arr(pn.nvar, lv, w)] * 3 + [arr(lv, pn.nvar)] * 3,
        in_specs=[vm] * len(got),
        compiler_params=small,
        name="place",
    )(*got)
    return tuple(jnp.transpose(o, (1, 0, 2)) for o in outs[:3]) + tuple(outs[3:])


def plain(pn, pred, truth, norm, flag, rows):
    band = lax.axis_index("lat")
    ids = jnp.arange(pn.lats, dtype=jnp.int32)
    first = jnp.sum(jnp.where(ids < band, rows, 0))
    count = jnp.sum(jnp.where(ids == band, rows, 0))
    slot = jnp.arange(pn.width, dtype=jnp.int32)
    inside = slot < count
    angles = jnp.pi * jnp.arange(pn.lat_total, dtype=jnp.float32) / (pn.lat_total - 1)
    angle = jnp.pi * (first + slot).astype(jnp.float32) / (pn.lat_total - 1)
    weight = jnp.where(inside, jnp.sin(angle) * pn.lat_total / jnp.sum(jnp.sin(angles)), 0.0)
    keep = flag.astype(jnp.float32) * inside.astype(jnp.float32)[None, :]
    t = truth - norm
    f = pred - norm[None]
    e = f - t[None]
    k = keep[None, None]
    sums = jnp.concatenate(
        [
            jnp.sum(k * e * e, axis=2),
            jnp.sum(k * e, axis=2),
            jnp.sum(k * f * t[None], axis=2),
            jnp.sum(k * f * f, axis=2),
            jnp.sum(k * t[None] * t[None], axis=2),
        ],
        axis=0,
    )
    grand = lax.psum(jnp.sum(sums * weight, axis=2), ("lat", "lon"))
    zonal = lax.psum(sums, "lon")

    def finish(s, n):
        parts = [s[m * pn.leads:(m + 1) * pn.leads] for m in range(4)]
        return metrics(*parts, s[4 * pn.leads:], n)

    mse, off, skill = finish(zonal, float(pn.lon_total))
    gm, go, gs = finish(grand, float(pn.lat_total * pn.lon_total))
    return mse, off, skill, jnp.sqrt(jnp.maximum(gm, FLOOR)), go, gs


def local(pred, truth, norm, flag, rows):
    leads, nvar, nlon, width = pred.shape
    pn = Plan(leads, nvar, nlon, width, lax.axis_size("lat"), lax.axis_size("lon"))
    return (fast if pn.fits() else plain)(pn, pred, truth, norm, flag, rows)


def solution(mesh):
    in_specs = (
        P(None, None, "lon", "lat"),
        P(None, "lon", "lat"),
        P(None, "lon", "lat"),
        P("lon", "lat"),
        P(),
    )
    out_specs = (P(None, None, "lat"), P(None, None, "lat"), P(None, None, "lat"), P(), P(), P())
    return jax.shard_map(local, mesh=mesh, in_specs=in_specs, out_specs=out_specs, check_vma=False)
```

```python
import functools
import math

import jax
import jax.numpy as jnp
import numpy as np
from jax import lax
from jax.experimental import pallas as pl
from jax.experimental.pallas import tpu as pltpu
from jax.sharding import PartitionSpec as P


MEAN_ROWS = 90
FLOOR = 0.1
SUB = 8
UNROLL = 9
PIECES = 3
NEAR = (2, 1, 3)
BACK = (3, 2, 1)


def quarter_of(pn, lon):
    return lax.rem(lon, pn.quad) ^ (2 * (lon // pn.quad))


class Plan:
    def __init__(self, leads, nvar, nlon, width, lats, lons):
        self.leads, self.nvar, self.nlon, self.width = leads, nvar, nlon, width
        self.lats, self.lons = lats, lons
        self.lat_total = MEAN_ROWS * lats + 1
        self.lon_total = nlon * lons
        self.quad = 4
        self.groups = nvar // SUB
        self.chunks = self.groups // self.quad
        self.top = self.groups * SUB
        self.extra = nvar - self.top
        self.sums = 4 * leads + 1
        self.xrow = self.sums * SUB
        self.rrows = self.chunks * self.xrow + 5 * self.extra
        self.prow = SUB * leads
        self.grow0 = self.chunks * 3 * self.prow
        self.grow1 = self.grow0 + 3 * self.extra

    def fits(self):
        return (
            self.lons == 2 * self.quad
            and self.chunks == 2
            and self.groups == self.chunks * self.quad
            and self.extra > 0
            and self.leads == self.quad
            and self.width == 128
        )


def sums_kernel(pn, pred, truth, norm, flag, rows, *refs):
    msgs = refs[:pn.quad]
    acc, wout, vp, vt, vn, vf, sp, keep, sem = refs[pn.quad:]
    w, lv = pn.width, pn.leads
    per = pn.nlon * lv
    groups = [(pn.top, pn.extra)] + [(SUB * g, SUB) for g in range(pn.groups)]
    cuts = [pn.nlon * i // PIECES for i in range(PIECES + 1)]
    pieces = [(v, n, 0, pn.nlon) for v, n in groups[:-1]]
    pieces += [groups[-1] + (lo, hi) for lo, hi in zip(cuts, cuts[1:])]
    copies = [
        pltpu.make_async_copy(rows, sp, sem.at[0]),
        pltpu.make_async_copy(flag, vf, sem.at[1]),
    ]
    for i, (v, n, lo, hi) in enumerate(pieces):
        var, lon = pl.ds(v, n), pl.ds(lo, hi - lo)
        copies += [
            pltpu.make_async_copy(norm.at[lon, var], vn.at[lon, var], sem.at[3 * i + 2]),
            pltpu.make_async_copy(truth.at[lon, var], vt.at[lon, var], sem.at[3 * i + 3]),
            pltpu.make_async_copy(pred.at[var, lon], vp.at[var, lon], sem.at[3 * i + 4]),
        ]
    for c in copies:
        c.start()
    for j in range(pn.sums):
        acc[j, pl.ds(pn.top, SUB), :] = jnp.zeros((SUB, w), jnp.float32)
    me_lat = lax.axis_index("lat")
    quarter = quarter_of(pn, lax.axis_index("lon"))
    copies[0].wait()
    first = jnp.int32(0)
    for b in range(pn.lats):
        first = first + jnp.where(b < me_lat, sp[b], 0)
    slot = lax.broadcasted_iota(jnp.int32, (SUB, w), 1)
    inside = slot < sp[me_lat]
    row = first + slot
    fold = jnp.minimum(row, pn.lat_total - 1 - row).astype(jnp.float32)
    x = fold * np.float32(math.pi / (pn.lat_total - 1))
    x2 = x * x
    poly = jnp.full_like(x, 1.0 / math.factorial(13))
    for d in (11, 9, 7, 5, 3, 1):
        poly = poly * x2 * (-1.0) + 1.0 / math.factorial(d)
    norms = float(np.sum(np.sin(np.pi * np.arange(pn.lat_total) / (pn.lat_total - 1))))
    wout[...] = jnp.where(inside, poly * x * np.float32(pn.lat_total / norms), 0.0)
    copies[1].wait()
    keep[...] = jnp.where(inside[0:1], vf[...], 0).astype(jnp.float32)
    flat = vp.reshape(pn.nvar * per, w)
    for i, (v, n, lo, hi) in enumerate(pieces):
        for c in copies[3 * i + 2:3 * i + 5]:
            c.wait()

        def body(l, c, v=v, n=n):
            k = keep[pl.ds(l, n, stride=0), :]
            a = vn[l, pl.ds(v, n), :]
            t = (vt[l, pl.ds(v, n), :] - a) * k
            a = a * k
            out = []
            for q in range(lv):
                f = flat[pl.ds(v * per + l * lv + q, n, stride=per), :] * k - a
                e = f - t
                out.append((c[q] + e * e, c[lv + q] + e, c[2 * lv + q] + f * t, c[3 * lv + q] + f * f))
            return tuple(out[q][m] for m in range(4) for q in range(lv)) + (c[4 * lv] + t * t,)

        if lo == 0:
            total = (jnp.zeros((n, w), jnp.float32),) * pn.sums
        total = lax.fori_loop(lo, hi, body, total, unroll=UNROLL if hi - lo == pn.nlon else hi - lo)
        if hi == pn.nlon:
            for j in range(pn.sums):
                acc[j, pl.ds(v, n), :] = total[j]
    for c in range(pn.chunks):
        for k in range(pn.quad):
            p = quarter ^ k
            base = pl.multiple_of(SUB * (pn.chunks * p + c), SUB)
            for j in range(pn.sums):
                msgs[k][pl.ds(c * pn.xrow + j * SUB, SUB), :] = acc[j, pl.ds(base, SUB), :]
    for k in range(pn.quad):
        p = quarter ^ k
        for m in range(5):
            j = m * lv + (p if m < 4 else 0)
            msgs[k][pl.ds(pn.chunks * pn.xrow + m * pn.extra, pn.extra), :] = acc[j, pl.ds(pn.top, pn.extra), :]


def weigh_kernel(pn, wt, acc, gout):
    gout[...] = jnp.zeros((pn.sums, pn.width), jnp.float32)
    for j in range(pn.sums):
        d = lax.dot_general(
            wt[...],
            acc[j],
            (((1,), (1,)), ((), ())),
            precision=lax.Precision.HIGHEST,
            preferred_element_type=jnp.float32,
        )
        gout[pl.ds(j, 1), pl.ds(0, pn.top + SUB)] = d[0:1]


def add_kernel(pn, own, r1, r2, r3, g, out):
    out[pl.ds(0, pn.rrows), :] = (own[...] + r1[...]) + (r2[...] + r3[...])
    out[pl.ds(pn.rrows, pn.sums), :] = g[...]


def metrics(sq, off, pr, sp, tt, n):
    skill = (pr / n) / jnp.sqrt(jnp.maximum(sp / n, FLOOR) * jnp.maximum(tt / n, FLOOR))
    return sq / n, off / n, skill


def final_kernel(pn, own, far, out):
    n = np.float32(pn.lon_total)
    lv = pn.leads

    def rows(r, m):
        return own[pl.ds(r, m), :] + far[pl.ds(r, m), :]

    for c in range(pn.chunks):
        at, to = c * pn.xrow, c * 3 * pn.prow
        tt = rows(at + 4 * lv * SUB, SUB)
        for q in range(lv):
            vals = metrics(*(rows(at + (d * lv + q) * SUB, SUB) for d in range(4)), tt, n)
            for i in range(3):
                out[pl.ds(to + i * pn.prow + q, SUB, stride=lv), :] = vals[i]
    x = pn.chunks * pn.xrow
    vals = metrics(*(rows(x + m * pn.extra, pn.extra) for m in range(5)), n)
    for i in range(3):
        out[pl.ds(pn.grow0 + i * pn.extra, pn.extra), :] = vals[i]
    out[pl.ds(pn.grow1, pn.sums), :] = rows(pn.rrows, pn.sums)


def place_kernel(pn, *refs):
    lv = pn.leads
    quarter = quarter_of(pn, lax.axis_index("lon"))
    got, outs = refs[:pn.quad], refs[pn.quad:]
    flats = [outs[i].reshape(pn.nvar * lv, pn.width) for i in range(3)]
    for k in range(pn.quad):
        p = quarter ^ k
        for i in range(3):
            for c in range(pn.chunks):
                base = pl.multiple_of((pn.chunks * p + c) * pn.prow, SUB)
                flats[i][pl.ds(base, pn.prow), :] = got[k][pl.ds((3 * c + i) * pn.prow, pn.prow), :]
            flats[i][pl.ds(pn.top * lv + p, pn.extra, stride=lv), :] = got[k][
                pl.ds(pn.grow0 + i * pn.extra, pn.extra), :
            ]
    a, b, c, d = (r[pl.ds(pn.grow1, pn.sums), :] for r in got)
    g = (a + b) + (c + d)
    n = np.float32(pn.lat_total * pn.lon_total)
    mse, off, skill = metrics(*(g[m * lv:(m + 1) * lv] for m in range(4)), g[4 * lv:4 * lv + 1], n)
    outs[3][...] = jnp.sqrt(jnp.maximum(mse, FLOOR))[:, : pn.nvar]
    outs[4][...] = off[:, : pn.nvar]
    outs[5][...] = skill[:, : pn.nvar]


def fast(pn, pred, truth, norm, flag, rows):
    f32 = jnp.float32
    w, lv = pn.width, pn.leads
    vm = pl.BlockSpec(memory_space=pltpu.VMEM)
    hbm = pl.BlockSpec(memory_space=pltpu.HBM)
    pred = jnp.transpose(pred, (1, 2, 0, 3))
    truth = jnp.transpose(truth, (1, 0, 2))
    norm = jnp.transpose(norm, (1, 0, 2))
    large = pltpu.CompilerParams(vmem_limit_bytes=24 * 2**20)
    small = pltpu.CompilerParams(vmem_limit_bytes=8 * 2**20)

    def arr(*shape):
        return jax.ShapeDtypeStruct(shape, f32)

    def call(kernel, out, *args):
        return pl.pallas_call(
            kernel,
            out_shape=out,
            in_specs=[vm] * len(args),
            out_specs=jax.tree.map(lambda _: vm, out),
            compiler_params=small,
        )(*args)

    def swap(x, k):
        return lax.ppermute(x, "lon", [(i, i ^ k) for i in range(pn.lons)])

    inputs = [pltpu.with_memory_space_constraint(a, pltpu.HBM) for a in (pred, truth, norm, flag, rows)]
    *msgs, acc, wt = pl.pallas_call(
        functools.partial(sums_kernel, pn),
        out_shape=[arr(pn.rrows, w)] * pn.quad
        + [arr(pn.sums, pn.top + SUB, w), arr(SUB, w)],
        in_specs=[hbm] * 5,
        out_specs=[vm] * (pn.quad + 2),
        scratch_shapes=[
            pltpu.VMEM(pred.shape, f32),
            pltpu.VMEM(truth.shape, f32),
            pltpu.VMEM(norm.shape, f32),
            pltpu.VMEM(flag.shape, jnp.int32),
            pltpu.SMEM(rows.shape, jnp.int32),
            pltpu.VMEM(flag.shape, f32),
            pltpu.SemaphoreType.DMA((2 + 3 * (pn.groups + PIECES),)),
        ],
        compiler_params=large,
        name="sums",
    )(*inputs)
    near = {k: swap(msgs[k], k) for k in NEAR}
    g = call(functools.partial(weigh_kernel, pn), arr(pn.sums, w), wt, acc)
    step = 1
    while step < pn.lats:
        g = g + lax.ppermute(g, "lat", [(i, i ^ step) for i in range(pn.lats)])
        step *= 2
    part = call(
        functools.partial(add_kernel, pn), arr(pn.rrows + pn.sums, w),
        msgs[0], near[1], near[2], near[3], g,
    )
    far = swap(part, pn.quad ^ 2)
    done = call(functools.partial(final_kernel, pn), arr(pn.grow1 + pn.sums, w), part, far)
    there = {k: swap(done, k) for k in BACK}
    got = [done, there[1], there[2], there[3]]
    outs = pl.pallas_call(
        functools.partial(place_kernel, pn),
        out_shape=[arr(pn.nvar, lv, w)] * 3 + [arr(lv, pn.nvar)] * 3,
        in_specs=[vm] * len(got),
        compiler_params=small,
        name="place",
    )(*got)
    return tuple(jnp.transpose(o, (1, 0, 2)) for o in outs[:3]) + tuple(outs[3:])


def plain(pn, pred, truth, norm, flag, rows):
    band = lax.axis_index("lat")
    ids = jnp.arange(pn.lats, dtype=jnp.int32)
    first = jnp.sum(jnp.where(ids < band, rows, 0))
    count = jnp.sum(jnp.where(ids == band, rows, 0))
    slot = jnp.arange(pn.width, dtype=jnp.int32)
    inside = slot < count
    angles = jnp.pi * jnp.arange(pn.lat_total, dtype=jnp.float32) / (pn.lat_total - 1)
    angle = jnp.pi * (first + slot).astype(jnp.float32) / (pn.lat_total - 1)
    weight = jnp.where(inside, jnp.sin(angle) * pn.lat_total / jnp.sum(jnp.sin(angles)), 0.0)
    keep = flag.astype(jnp.float32) * inside.astype(jnp.float32)[None, :]
    t = truth - norm
    f = pred - norm[None]
    e = f - t[None]
    k = keep[None, None]
    sums = jnp.concatenate(
        [
            jnp.sum(k * e * e, axis=2),
            jnp.sum(k * e, axis=2),
            jnp.sum(k * f * t[None], axis=2),
            jnp.sum(k * f * f, axis=2),
            jnp.sum(k * t[None] * t[None], axis=2),
        ],
        axis=0,
    )
    grand = lax.psum(jnp.sum(sums * weight, axis=2), ("lat", "lon"))
    zonal = lax.psum(sums, "lon")

    def finish(s, n):
        parts = [s[m * pn.leads:(m + 1) * pn.leads] for m in range(4)]
        return metrics(*parts, s[4 * pn.leads:], n)

    mse, off, skill = finish(zonal, float(pn.lon_total))
    gm, go, gs = finish(grand, float(pn.lat_total * pn.lon_total))
    return mse, off, skill, jnp.sqrt(jnp.maximum(gm, FLOOR)), go, gs


def local(pred, truth, norm, flag, rows):
    leads, nvar, nlon, width = pred.shape
    pn = Plan(leads, nvar, nlon, width, lax.axis_size("lat"), lax.axis_size("lon"))
    return (fast if pn.fits() else plain)(pn, pred, truth, norm, flag, rows)


def solution(mesh):
    in_specs = (
        P(None, None, "lon", "lat"),
        P(None, "lon", "lat"),
        P(None, "lon", "lat"),
        P("lon", "lat"),
        P(),
    )
    out_specs = (P(None, None, "lat"), P(None, None, "lat"), P(None, None, "lat"), P(), P(), P())
    return jax.shard_map(local, mesh=mesh, in_specs=in_specs, out_specs=out_specs, check_vma=False)
```

```python
import functools
import math

import jax
import jax.numpy as jnp
import numpy as np
from jax import lax
from jax.experimental import pallas as pl
from jax.experimental.pallas import tpu as pltpu
from jax.sharding import PartitionSpec as P


MEAN_ROWS = 90
FLOOR = 0.1
SUB = 8
UNROLL = 9
PIECES = 3
NEAR = (2, 1, 3)
BACK = (3, 2, 1)


def quarter_of(pn, lon):
    return lax.rem(lon, pn.quad) ^ (2 * (lon // pn.quad))


class Plan:
    def __init__(self, leads, nvar, nlon, width, lats, lons):
        self.leads, self.nvar, self.nlon, self.width = leads, nvar, nlon, width
        self.lats, self.lons = lats, lons
        self.lat_total = MEAN_ROWS * lats + 1
        self.lon_total = nlon * lons
        self.quad = 4
        self.groups = nvar // SUB
        self.chunks = self.groups // self.quad
        self.top = self.groups * SUB
        self.extra = nvar - self.top
        self.sums = 4 * leads + 1
        self.spare = width - nvar
        self.packed = self.sums - 2
        self.xrow = self.sums * SUB
        self.rrows = self.chunks * self.xrow + 5 * self.extra
        self.prow = SUB * leads
        self.grow0 = self.chunks * 3 * self.prow
        self.grow1 = self.grow0 + 3 * self.extra

    def fits(self):
        return (
            self.lons == 2 * self.quad
            and self.chunks == 2
            and self.groups == self.chunks * self.quad
            and self.extra > 0
            and self.leads == self.quad
            and self.width == 128
            and self.spare < self.nvar <= 2 * self.spare
        )


def sums_kernel(pn, pred, truth, norm, flag, rows, *refs):
    msgs = refs[:pn.quad]
    acc, wout, vp, vt, vn, vf, sp, keep, sem = refs[pn.quad:]
    w, lv = pn.width, pn.leads
    per = pn.nlon * lv
    groups = [(pn.top, pn.extra)] + [(SUB * g, SUB) for g in range(pn.groups)]
    cuts = [pn.nlon * i // PIECES for i in range(PIECES + 1)]
    pieces = [(v, n, 0, pn.nlon) for v, n in groups[:-1]]
    pieces += [groups[-1] + (lo, hi) for lo, hi in zip(cuts, cuts[1:])]
    copies = [
        pltpu.make_async_copy(rows, sp, sem.at[0]),
        pltpu.make_async_copy(flag, vf, sem.at[1]),
    ]
    for i, (v, n, lo, hi) in enumerate(pieces):
        var, lon = pl.ds(v, n), pl.ds(lo, hi - lo)
        copies += [
            pltpu.make_async_copy(norm.at[lon, var], vn.at[lon, var], sem.at[3 * i + 2]),
            pltpu.make_async_copy(truth.at[lon, var], vt.at[lon, var], sem.at[3 * i + 3]),
            pltpu.make_async_copy(pred.at[var, lon], vp.at[var, lon], sem.at[3 * i + 4]),
        ]
    for c in copies:
        c.start()
    for j in range(pn.sums):
        acc[j, pl.ds(pn.top, SUB), :] = jnp.zeros((SUB, w), jnp.float32)
    me_lat = lax.axis_index("lat")
    quarter = quarter_of(pn, lax.axis_index("lon"))
    copies[0].wait()
    first = jnp.int32(0)
    for b in range(pn.lats):
        first = first + jnp.where(b < me_lat, sp[b], 0)
    slot = lax.broadcasted_iota(jnp.int32, (SUB, w), 1)
    inside = slot < sp[me_lat]
    row = first + slot
    fold = jnp.minimum(row, pn.lat_total - 1 - row).astype(jnp.float32)
    x = fold * np.float32(math.pi / (pn.lat_total - 1))
    x2 = x * x
    poly = jnp.full_like(x, 1.0 / math.factorial(13))
    for d in (11, 9, 7, 5, 3, 1):
        poly = poly * x2 * (-1.0) + 1.0 / math.factorial(d)
    norms = float(np.sum(np.sin(np.pi * np.arange(pn.lat_total) / (pn.lat_total - 1))))
    wout[...] = jnp.where(inside, poly * x * np.float32(pn.lat_total / norms), 0.0)
    copies[1].wait()
    keep[...] = jnp.where(inside[0:1], vf[...], 0).astype(jnp.float32)
    flat = vp.reshape(pn.nvar * per, w)
    for i, (v, n, lo, hi) in enumerate(pieces):
        for c in copies[3 * i + 2:3 * i + 5]:
            c.wait()

        def body(l, c, v=v, n=n):
            k = keep[pl.ds(l, n, stride=0), :]
            a = vn[l, pl.ds(v, n), :]
            t = (vt[l, pl.ds(v, n), :] - a) * k
            a = a * k
            out = []
            for q in range(lv):
                f = flat[pl.ds(v * per + l * lv + q, n, stride=per), :] * k - a
                e = f - t
                out.append((c[q] + e * e, c[lv + q] + e, c[2 * lv + q] + f * t, c[3 * lv + q] + f * f))
            return tuple(out[q][m] for m in range(4) for q in range(lv)) + (c[4 * lv] + t * t,)

        if lo == 0:
            total = (jnp.zeros((n, w), jnp.float32),) * pn.sums
        total = lax.fori_loop(lo, hi, body, total, unroll=UNROLL if hi - lo == pn.nlon else hi - lo)
        if hi == pn.nlon:
            for j in range(pn.sums):
                acc[j, pl.ds(v, n), :] = total[j]
    for c in range(pn.chunks):
        for k in range(pn.quad):
            p = quarter ^ k
            base = pl.multiple_of(SUB * (pn.chunks * p + c), SUB)
            for j in range(pn.sums):
                msgs[k][pl.ds(c * pn.xrow + j * SUB, SUB), :] = acc[j, pl.ds(base, SUB), :]
    for k in range(pn.quad):
        p = quarter ^ k
        for m in range(5):
            j = m * lv + (p if m < 4 else 0)
            msgs[k][pl.ds(pn.chunks * pn.xrow + m * pn.extra, pn.extra), :] = acc[j, pl.ds(pn.top, pn.extra), :]


def weigh_kernel(pn, wt, acc, gout):
    gout[...] = jnp.zeros((pn.packed, pn.width), jnp.float32)
    for j in range(pn.sums):
        d = lax.dot_general(
            wt[...],
            acc[j],
            (((1,), (1,)), ((), ())),
            precision=lax.Precision.HIGHEST,
            preferred_element_type=jnp.float32,
        )
        if j < pn.packed:
            gout[pl.ds(j, 1), pl.ds(0, pn.nvar)] = d[0:1, : pn.nvar]
        else:
            at = 2 * (j - pn.packed)
            gout[pl.ds(at, 1), pl.ds(pn.nvar, pn.spare)] = d[0:1, : pn.spare]
            gout[pl.ds(at + 1, 1), pl.ds(pn.nvar, pn.nvar - pn.spare)] = d[0:1, pn.spare:pn.nvar]


def add_kernel(pn, own, r1, r2, r3, g, out):
    out[pl.ds(0, pn.rrows), :] = (own[...] + r1[...]) + (r2[...] + r3[...])
    out[pl.ds(pn.rrows, pn.packed), :] = g[...]


def metrics(sq, off, pr, sp, tt, n):
    skill = (pr / n) / jnp.sqrt(jnp.maximum(sp / n, FLOOR) * jnp.maximum(tt / n, FLOOR))
    return sq / n, off / n, skill


def final_kernel(pn, own, far, out):
    n = np.float32(pn.lon_total)
    lv = pn.leads

    def rows(r, m):
        return own[pl.ds(r, m), :] + far[pl.ds(r, m), :]

    for c in range(pn.chunks):
        at, to = c * pn.xrow, c * 3 * pn.prow
        tt = rows(at + 4 * lv * SUB, SUB)
        for q in range(lv):
            vals = metrics(*(rows(at + (d * lv + q) * SUB, SUB) for d in range(4)), tt, n)
            for i in range(3):
                out[pl.ds(to + i * pn.prow + q, SUB, stride=lv), :] = vals[i]
    x = pn.chunks * pn.xrow
    vals = metrics(*(rows(x + m * pn.extra, pn.extra) for m in range(5)), n)
    for i in range(3):
        out[pl.ds(pn.grow0 + i * pn.extra, pn.extra), :] = vals[i]
    out[pl.ds(pn.grow1, pn.packed), :] = rows(pn.rrows, pn.packed)


def place_kernel(pn, *refs):
    lv = pn.leads
    quarter = quarter_of(pn, lax.axis_index("lon"))
    got, outs = refs[:pn.quad], refs[pn.quad:]
    flats = [outs[i].reshape(pn.nvar * lv, pn.width) for i in range(3)]
    for k in range(pn.quad):
        p = quarter ^ k
        for i in range(3):
            for c in range(pn.chunks):
                base = pl.multiple_of((pn.chunks * p + c) * pn.prow, SUB)
                flats[i][pl.ds(base, pn.prow), :] = got[k][pl.ds((3 * c + i) * pn.prow, pn.prow), :]
            flats[i][pl.ds(pn.top * lv + p, pn.extra, stride=lv), :] = got[k][
                pl.ds(pn.grow0 + i * pn.extra, pn.extra), :
            ]
    a, b, c, d = (r[pl.ds(pn.grow1, pn.packed), :] for r in got)
    g = (a + b) + (c + d)
    n = np.float32(pn.lat_total * pn.lon_total)
    v = pn.nvar
    late = [jnp.concatenate([g[i:i + 1, v:], g[i + 1:i + 2, v:2 * v - pn.spare]], axis=1) for i in (0, 2)]
    head = [g[m * lv:(m + 1) * lv, :v] for m in range(3)]
    spread = jnp.concatenate([g[3 * lv:pn.packed, :v], late[0]], axis=0)
    mse, off, skill = metrics(*head, spread, late[1], n)
    outs[3][...] = jnp.sqrt(jnp.maximum(mse, FLOOR))
    outs[4][...] = off
    outs[5][...] = skill


def fast(pn, pred, truth, norm, flag, rows):
    f32 = jnp.float32
    w, lv = pn.width, pn.leads
    vm = pl.BlockSpec(memory_space=pltpu.VMEM)
    hbm = pl.BlockSpec(memory_space=pltpu.HBM)
    pred = jnp.transpose(pred, (1, 2, 0, 3))
    truth = jnp.transpose(truth, (1, 0, 2))
    norm = jnp.transpose(norm, (1, 0, 2))
    large = pltpu.CompilerParams(vmem_limit_bytes=24 * 2**20)
    small = pltpu.CompilerParams(vmem_limit_bytes=8 * 2**20)

    def arr(*shape):
        return jax.ShapeDtypeStruct(shape, f32)

    def call(kernel, out, *args):
        return pl.pallas_call(
            kernel,
            out_shape=out,
            in_specs=[vm] * len(args),
            out_specs=jax.tree.map(lambda _: vm, out),
            compiler_params=small,
        )(*args)

    def swap(x, k):
        return lax.ppermute(x, "lon", [(i, i ^ k) for i in range(pn.lons)])

    inputs = [pltpu.with_memory_space_constraint(a, pltpu.HBM) for a in (pred, truth, norm, flag, rows)]
    *msgs, acc, wt = pl.pallas_call(
        functools.partial(sums_kernel, pn),
        out_shape=[arr(pn.rrows, w)] * pn.quad
        + [arr(pn.sums, pn.top + SUB, w), arr(SUB, w)],
        in_specs=[hbm] * 5,
        out_specs=[vm] * (pn.quad + 2),
        scratch_shapes=[
            pltpu.VMEM(pred.shape, f32),
            pltpu.VMEM(truth.shape, f32),
            pltpu.VMEM(norm.shape, f32),
            pltpu.VMEM(flag.shape, jnp.int32),
            pltpu.SMEM(rows.shape, jnp.int32),
            pltpu.VMEM(flag.shape, f32),
            pltpu.SemaphoreType.DMA((2 + 3 * (pn.groups + PIECES),)),
        ],
        compiler_params=large,
        name="sums",
    )(*inputs)
    near = {k: swap(msgs[k], k) for k in NEAR}
    g = call(functools.partial(weigh_kernel, pn), arr(pn.packed, w), wt, acc)
    step = 1
    while step < pn.lats:
        g = g + lax.ppermute(g, "lat", [(i, i ^ step) for i in range(pn.lats)])
        step *= 2
    part = call(
        functools.partial(add_kernel, pn), arr(pn.rrows + pn.packed, w),
        msgs[0], near[1], near[2], near[3], g,
    )
    far = swap(part, pn.quad ^ 2)
    done = call(functools.partial(final_kernel, pn), arr(pn.grow1 + pn.packed, w), part, far)
    there = {k: swap(done, k) for k in BACK}
    got = [done, there[1], there[2], there[3]]
    outs = pl.pallas_call(
        functools.partial(place_kernel, pn),
        out_shape=[arr(pn.nvar, lv, w)] * 3 + [arr(lv, pn.nvar)] * 3,
        in_specs=[vm] * len(got),
        compiler_params=small,
        name="place",
    )(*got)
    return tuple(jnp.transpose(o, (1, 0, 2)) for o in outs[:3]) + tuple(outs[3:])


def plain(pn, pred, truth, norm, flag, rows):
    band = lax.axis_index("lat")
    ids = jnp.arange(pn.lats, dtype=jnp.int32)
    first = jnp.sum(jnp.where(ids < band, rows, 0))
    count = jnp.sum(jnp.where(ids == band, rows, 0))
    slot = jnp.arange(pn.width, dtype=jnp.int32)
    inside = slot < count
    angles = jnp.pi * jnp.arange(pn.lat_total, dtype=jnp.float32) / (pn.lat_total - 1)
    angle = jnp.pi * (first + slot).astype(jnp.float32) / (pn.lat_total - 1)
    weight = jnp.where(inside, jnp.sin(angle) * pn.lat_total / jnp.sum(jnp.sin(angles)), 0.0)
    keep = flag.astype(jnp.float32) * inside.astype(jnp.float32)[None, :]
    t = truth - norm
    f = pred - norm[None]
    e = f - t[None]
    k = keep[None, None]
    sums = jnp.concatenate(
        [
            jnp.sum(k * e * e, axis=2),
            jnp.sum(k * e, axis=2),
            jnp.sum(k * f * t[None], axis=2),
            jnp.sum(k * f * f, axis=2),
            jnp.sum(k * t[None] * t[None], axis=2),
        ],
        axis=0,
    )
    grand = lax.psum(jnp.sum(sums * weight, axis=2), ("lat", "lon"))
    zonal = lax.psum(sums, "lon")

    def finish(s, n):
        parts = [s[m * pn.leads:(m + 1) * pn.leads] for m in range(4)]
        return metrics(*parts, s[4 * pn.leads:], n)

    mse, off, skill = finish(zonal, float(pn.lon_total))
    gm, go, gs = finish(grand, float(pn.lat_total * pn.lon_total))
    return mse, off, skill, jnp.sqrt(jnp.maximum(gm, FLOOR)), go, gs


def local(pred, truth, norm, flag, rows):
    leads, nvar, nlon, width = pred.shape
    pn = Plan(leads, nvar, nlon, width, lax.axis_size("lat"), lax.axis_size("lon"))
    return (fast if pn.fits() else plain)(pn, pred, truth, norm, flag, rows)


def solution(mesh):
    in_specs = (
        P(None, None, "lon", "lat"),
        P(None, "lon", "lat"),
        P(None, "lon", "lat"),
        P("lon", "lat"),
        P(),
    )
    out_specs = (P(None, None, "lat"), P(None, None, "lat"), P(None, None, "lat"), P(), P(), P())
    return jax.shard_map(local, mesh=mesh, in_specs=in_specs, out_specs=out_specs, check_vma=False)
```
